256 devices in a mesh: grp: 8 (over y, core), head: 32 (over z, x).
Axes of the slice: x: 4, y: 4, z: 8, core: 2. Of those that a mesh axis runs over, the one named last changes fastest.
Arguments:
- query_latent: bfloat16 [4096, 1536], P('grp'), may hold values from -6 to 6
- q_weight: bfloat16 [1536, 24576], P('grp', 'head'), may hold values from -0.15625 to 0.15625
- key_absorb: bfloat16 [128, 128, 512], P('head'), may hold values from -0.5 to 0.5
- value_up: bfloat16 [128, 512, 128], P('head'), may hold values from -0.25 to 0.25
- branch_latent: bfloat16 [8, 1536, 576], P('grp', 'head'), may hold values from -800 to 800, as said below
- lengths: int32 [8], P('grp'), may hold values from 512 to 1536, as said below
- row_depth: int32 [4096], P('grp'), may hold values from 1 to 1536
Outputs:
- attended: bfloat16 [4096, 16384], P('grp', 'head')
The draws below stay inside these ranges and needn't reach their ends.
Inputs may be any that keep to these rules, and one draw needn't show every extreme that they name: `lengths`: every group has between 512 and 1536 live positions; some group has exactly 1536 and some other exactly 512. `branch_latent`: latent entries of order one.
All inputs are finite; a program needn't handle non-finite values.
Results may differ from the reference program's by a relative error of at most 0.012.
Values may be sent and summed in bfloat16 or wider, within the bound.
No kernel may reach another device: no remote copies, remote signals or barrier semaphores. Data moves between devices by JAX's collectives and lax.ppermute only.
A program may use at most 64 MiB of HBM per device.

```python
import jax
import jax.numpy as jnp
from jax import lax

QRANK = 1536
HEADS = 128
NOPE = 128
ROPE = 64
KVR = 512
VDIM = 128
ROWS_GRP = 512
LMAX = 1536
GROUPS = 8
ROWS = 4096


def draw_lengths(key, part):
    inner = jax.random.fold_in(key, 11)
    first, second = jax.random.split(inner)
    base = jax.random.randint(first, (GROUPS,), LMAX // 3, LMAX + 1)
    order = jax.random.permutation(second, GROUPS)
    base = base.at[order[0]].set(LMAX)
    base = base.at[order[1]].set(LMAX // 3)
    return base.astype(jnp.int32)


def draw_branch_latent(key, part):
    inner = jax.random.fold_in(key, 23)
    first = jax.random.fold_in(inner, 0)
    shape = (GROUPS, LMAX, KVR + ROPE)
    base = jnp.clip(jax.random.normal(first, shape, jnp.float32), -6.0, 6.0)
    return base.astype(jnp.bfloat16)


def touch_ends(array, rng, low, largest):
    extent = array.shape
    spot = [jax.random.randint(jax.random.fold_in(rng, axis), (), 0, extent[axis]) for axis in range(len(extent))]
    array = array.at[tuple(spot)].set(low)
    longest = extent.index(max(extent))
    spot[longest] = (spot[longest] + 1) % extent[longest]
    return array.at[tuple(spot)].set(largest)


def shard_levels(stream_key, extent, cuts, smallest, high):
    def one(axis_at, shards_of):
        draws = jax.random.uniform(jax.random.fold_in(jax.random.fold_in(stream_key, 6), axis_at), (shards_of,), jnp.float32, smallest / len(cuts), high / len(cuts))
        return jnp.repeat(jnp.exp(draws), extent[axis_at] // shards_of).reshape((-1,) + (1,) * (len(extent) - axis_at - 1))

    factor_of = one(*cuts[0])
    for cut in cuts[1:]:
        factor_of = factor_of * one(*cut)
    return factor_of


def noise(own_key, shape, spread, reach, cuts=(), held_as=jnp.bfloat16):
    gain = shard_levels(own_key, shape, cuts, -0.22, 0.18) if cuts else 1.0
    drawn = jax.random.normal(own_key, shape, jnp.float32) * spread * gain
    return jnp.minimum(jnp.maximum(drawn, -reach), reach).astype(held_as)


def setup_inputs(seed: int = 0) -> dict:
    keys = jax.random.split(jax.random.key(seed), 8)
    query_latent = noise(keys[0], (ROWS, QRANK), 1.0, 6.0, ((0, 8),))
    q_weight = noise(keys[1], (QRANK, HEADS * (NOPE + ROPE)), QRANK ** -0.5, 0.15625, ((0, 8), (1, 32)))
    key_absorb = noise(keys[2], (HEADS, NOPE, KVR), NOPE ** -0.5, 0.5, ((0, 32),))
    value_up = noise(keys[3], (HEADS, KVR, VDIM), KVR ** -0.5, 0.25, ((0, 32),))
    branch_latent = draw_branch_latent(jax.random.fold_in(keys[7], 71), 0)
    lengths = draw_lengths(jax.random.fold_in(keys[7], 71), 0)
    row_depth = touch_ends(jax.random.randint(keys[6], (ROWS,), 1, LMAX + 1), jax.random.fold_in(keys[6], 1), 1, LMAX).astype(jnp.int32)
    return dict(query_latent=query_latent, q_weight=q_weight, key_absorb=key_absorb, value_up=value_up, branch_latent=branch_latent, lengths=lengths, row_depth=row_depth)


def attend(queries, depth, limit, latent, scale):
    count = queries.shape[0]
    block = 512 if count % 512 == 0 else count
    positions = jnp.arange(latent.shape[0], dtype=jnp.int32)
    values = latent[:, :KVR]
    query_blocks = queries.reshape(count // block, block, queries.shape[1])
    depth_blocks = jnp.minimum(depth, limit).reshape(count // block, block)

    def one_block(pair):
        query_rows, seen = pair
        score = lax.dot_general(query_rows, latent, (((1,), (1,)), ((), ())), preferred_element_type=jnp.float32) * scale
        score = jnp.where(positions[None, :] < seen[:, None], score, jnp.float32(-1e30))
        peak = jnp.max(score, axis=1, keepdims=True)
        expo = jnp.exp(score - peak)
        weights = (expo / jnp.sum(expo, axis=1, keepdims=True)).astype(jnp.bfloat16)
        return jnp.dot(weights, values, preferred_element_type=jnp.float32).astype(jnp.bfloat16)

    result = lax.map(one_block, (query_blocks, depth_blocks))
    return result.reshape(count, values.shape[1])


def reference(query_latent, q_weight, key_absorb, value_up, branch_latent, lengths, row_depth):
    scale = jnp.float32((NOPE + ROPE) ** -0.5)
    query = jnp.dot(query_latent, q_weight, preferred_element_type=jnp.float32).astype(jnp.bfloat16)
    query = query.reshape(ROWS, HEADS, NOPE + ROPE)
    q_lat = jnp.einsum("rhd,hdc->rhc", query[:, :, :NOPE].astype(jnp.float32), key_absorb.astype(jnp.float32)).astype(jnp.bfloat16)
    q_abs = jnp.concatenate([q_lat, query[:, :, NOPE:]], axis=2)
    grouped = q_abs.reshape(GROUPS, ROWS_GRP * HEADS, KVR + ROPE)
    depth = jnp.repeat(row_depth.reshape(GROUPS, ROWS_GRP), HEADS, axis=1)

    def per_group(items):
        queries, seen, limit, latent = items
        return attend(queries, seen, limit, latent, scale)

    context = lax.map(per_group, (grouped, depth, lengths, branch_latent))
    context = context.reshape(ROWS, HEADS, KVR)
    result = jnp.einsum("rhc,hcv->rhv", context.astype(jnp.float32), value_up.astype(jnp.float32))
    return result.reshape(ROWS, HEADS * VDIM).astype(jnp.bfloat16)
```

```python
import math

import jax
import jax.numpy as jnp
from jax import lax
from jax.experimental import pallas as pl
from jax.experimental.pallas import tpu as pltpu
from jax.sharding import Mesh
from jax.sharding import PartitionSpec as P


NOPE = 128
ROPE = 64
KVR = 512
VDIM = 128
WIDTH = KVR + ROPE
QDIM = NOPE + ROPE
LMAX = 1536
ROWS = 512
HEADS = 4
RB = 128
NRB = ROWS // RB
M = RB * HEADS
PB = 256
NPB = LMAX // PB
MASKED = -1e30
SCALE2 = (NOPE + ROPE) ** (-0.5) * math.log2(math.e)
F32 = jnp.float32
BF16 = jnp.bfloat16
NT = (((1,), (1,)), ((), ()))


def iota(shape, dim):
    return lax.broadcasted_iota(jnp.int32, shape, dim).astype(F32)


def weight_row(place_ref, dy, other):
    core = 1 - place_ref[1] if other else place_ref[1]
    return pl.multiple_of(lax.rem(place_ref[0] + dy, 4) * 384 + core * 192, 64)


def project_body(limit_ref, place_ref, ql_hbm, own_hbm, depth_ref, *refs):
    pieces = refs[: len(WEIGHT_PIECES)]
    absorb_hbm, out_ref, seen_ref, rank_ref, weight, ordered, ql_ref, absorb_ref, arrived = refs[len(WEIGHT_PIECES) :]
    fetch_ql = pltpu.make_async_copy(ql_hbm, ql_ref, arrived.at[0])
    fetch_ql.start()
    fetch_absorb = pltpu.make_async_copy(absorb_hbm, absorb_ref, arrived.at[1])
    fetch_absorb.start()
    fetch_own = pltpu.make_async_copy(own_hbm, weight.at[pl.ds(weight_row(place_ref, 0, False), 192), :], arrived.at[2])
    fetch_own.start()
    seen = jnp.minimum(depth_ref[...], limit_ref[0]).astype(F32)
    rows = iota((ROWS, ROWS), 0)
    cols = iota((ROWS, ROWS), 1)
    key_row = jnp.broadcast_to(seen * ROWS, (ROWS, ROWS)) + cols
    diagonal = rows == cols
    key_col = jnp.sum(jnp.where(diagonal, key_row, 0.0), axis=1, keepdims=True)
    below = jnp.where(key_col < key_row, 1.0, 0.0)
    rank_row = jnp.sum(below, axis=0, keepdims=True)
    rank_ref[...] = jnp.sum(jnp.where(key_row < key_col, 1.0, 0.0), axis=1, keepdims=True)
    chosen = rows == rank_row
    seen_ref[...] = jnp.sum(jnp.where(chosen, seen, 0.0), axis=1, keepdims=True)
    order = jnp.where(chosen, 1.0, 0.0).astype(BF16)
    fetch_ql.wait()
    ordered[...] = jnp.dot(order, ql_ref[...], preferred_element_type=F32).astype(BF16)
    for ref, (dy, other) in zip(pieces, WEIGHT_PIECES, strict=True):
        weight[pl.ds(weight_row(place_ref, dy, other), 192), :] = ref[...]
    fetch_own.wait()
    query = jnp.dot(ordered[...], weight[...], preferred_element_type=F32).astype(BF16)
    fetch_absorb.wait()
    for h in range(HEADS):
        nope = query[:, h * QDIM : h * QDIM + NOPE]
        rope = query[:, h * QDIM + NOPE : (h + 1) * QDIM]
        lat = jnp.dot(nope, absorb_ref[h], preferred_element_type=F32).astype(BF16)
        for b in range(NRB):
            out_ref[b, h, :, :KVR] = lat[b * RB : (b + 1) * RB]
            out_ref[b, h, :, KVR:] = rope[b * RB : (b + 1) * RB]


def join_body(*refs):
    row = 0
    for ref in refs[:-1]:
        refs[-1][row : row + ref.shape[0], :] = ref[...]
        row += ref.shape[0]


def attend_body(n_pieces, table, place_ref, query_ref, seen_ref, rank_ref, value_ref, *refs):
    pieces = refs[:n_pieces]
    out_ref, latent, score, seen_wide, peak, total, acc, result = refs[n_pieces:]
    z, x = place_ref[2], place_ref[3]
    for ref, blocks in zip(pieces, table, strict=True):
        for row, size, dz, dx, skip in blocks:
            start = (lax.rem(z + dz, 8) * 4 + lax.rem(x + dx, 4)) * 48 + skip
            latent[pl.ds(pl.multiple_of(start, 8), size), :] = ref[row : row + size, :]
    lanes = iota((M, 128), 1)

    def block(b, carry):
        base = pl.multiple_of(b * RB, RB)
        seen = jnp.broadcast_to(seen_ref[pl.ds(base, RB), :], (RB, 128))
        most = jnp.max(seen)
        count = (most.astype(jnp.int32) + (PB - 1)) // PB
        seen_wide[...] = jnp.concatenate([seen] * HEADS, axis=0)

        def scores(i, first):
            start = i * PB
            s = lax.dot_general(
                query_ref[b].reshape(M, WIDTH), latent[pl.ds(start, PB), :], NT, preferred_element_type=F32
            )
            halves = []
            for j in range(PB // 128):
                at = lanes + float(start + 128 * j)
                half = jnp.where(at < seen_wide[...], s[:, 128 * j : 128 * (j + 1)], MASKED)
                score[i, :, 128 * j : 128 * (j + 1)] = half
                halves.append(half)
            best = halves[0]
            for half in halves[1:]:
                best = jnp.maximum(best, half)
            peak[...] = best if first else jnp.maximum(peak[...], best)

        def values(i, first):
            start = i * PB
            parts = [
                jnp.exp2((score[i, :, 128 * j : 128 * (j + 1)] - peak[...]) * SCALE2) for j in range(PB // 128)
            ]
            add = parts[0]
            for part in parts[1:]:
                add = add + part
            total[...] = add if first else total[...] + add
            weights = jnp.concatenate([part.astype(BF16) for part in parts], axis=1)
            more = jnp.dot(weights, latent[pl.ds(start, PB), :KVR], preferred_element_type=F32)
            acc[...] = more if first else acc[...] + more

        def widen():
            peak[...] = jnp.broadcast_to(jnp.max(peak[...], axis=1, keepdims=True), (M, 128))

        def finish():
            inverse = 1.0 / jnp.sum(total[...], axis=1, keepdims=True)
            context = (acc[...] * inverse).astype(BF16)
            for h in range(HEADS):
                result[pl.ds(base, RB), h * VDIM : (h + 1) * VDIM] = jnp.dot(
                    context[h * RB : (h + 1) * RB], value_ref[h], preferred_element_type=F32
                ).astype(BF16)

        for n in range(1, NPB + 1):
            @pl.when(count == n)
            def _():
                for i in range(n):
                    scores(i, i == 0)
                widen()
                for i in range(n):
                    values(i, i == 0)
                finish()
        return carry

    lax.fori_loop(0, NRB, block, 0)
    back = jnp.where(iota((ROWS, ROWS), 1) == rank_ref[...], 1.0, 0.0).astype(BF16)
    out_ref[...] = jnp.dot(back, result[...], preferred_element_type=F32).astype(BF16)


SMEM = pl.BlockSpec(memory_space=pltpu.SMEM)
VMEM = pl.BlockSpec(memory_space=pltpu.VMEM)
HBM = pl.BlockSpec(memory_space=pltpu.HBM)


def call(body, smem, vmem, outs, scratch, flops, limit, far=()):
    one = len(outs) == 1
    return pl.pallas_call(
        body,
        in_specs=[SMEM] * len(smem) + [HBM if i in far else VMEM for i in range(len(vmem))],
        out_specs=VMEM if one else [VMEM] * len(outs),
        out_shape=outs[0] if one else outs,
        scratch_shapes=scratch,
        compiler_params=pltpu.CompilerParams(vmem_limit_bytes=limit),
        cost_estimate=pl.CostEstimate(flops=flops, transcendentals=0, bytes_accessed=1 << 20),
    )(*smem, *vmem)


def in_hbm(value):
    return pltpu.with_memory_space_constraint(value, pltpu.HBM)


def project(limit, place, depth, ql, pieces, absorb):
    column = jax.ShapeDtypeStruct((ROWS, 1), F32)
    return call(
        project_body, [limit, place], [in_hbm(ql), in_hbm(pieces[0]), depth, *pieces[1:], in_hbm(absorb)],
        [jax.ShapeDtypeStruct((NRB, HEADS, RB, WIDTH), BF16), column, column],
        [
            pltpu.VMEM((1536, HEADS * QDIM), BF16),
            pltpu.VMEM((ROWS, 1536), BF16),
            pltpu.VMEM((ROWS, 1536), BF16),
            pltpu.VMEM((HEADS, NOPE, KVR), BF16),
            pltpu.SemaphoreType.DMA((3,)),
        ],
        2 * ROWS * 1536 * (768 + ROWS) + 2 * ROWS * HEADS * NOPE * KVR, 24 << 20, (0, 1, len(pieces) + 2),
    )


def join(*pieces):
    count = sum(piece.shape[0] for piece in pieces)
    return call(join_body, [], list(pieces), [jax.ShapeDtypeStruct((count, WIDTH), BF16)], [], 1 << 20, 4 << 20)


def attend(place, query, seen, rank, value_up, pieces, table):
    body = lambda *refs: attend_body(len(pieces), table, *refs)
    return call(
        body, [place], [query, seen, rank, value_up, *pieces],
        [jax.ShapeDtypeStruct((ROWS, HEADS * VDIM), BF16)],
        [
            pltpu.VMEM((LMAX, WIDTH), BF16),
            pltpu.VMEM((NPB, M, PB), F32),
            pltpu.VMEM((M, 128), F32),
            pltpu.VMEM((M, 128), F32),
            pltpu.VMEM((M, 128), F32),
            pltpu.VMEM((M, KVR), F32),
            pltpu.VMEM((ROWS, HEADS * VDIM), BF16),
        ],
        2 * ROWS * HEADS * LMAX * (WIDTH + KVR), 30 << 20,
    )


def send(value, axis, size, step):
    return lax.ppermute(value, axis, [(i, (i + step) % size) for i in range(size)])


def weight_pieces(w):
    up = send(w, "y", 4, 1)
    down = send(w, "y", 4, -1)
    own2 = send(w, "core", 2, 1)
    far = send(up, "y", 4, 1)
    up2 = send(up, "core", 2, 1)
    down2 = send(down, "core", 2, 1)
    far2 = send(far, "core", 2, 1)
    return (w, up, down, far, own2, up2, down2, far2)


WEIGHT_PIECES = tuple((dy, other) for other in (False, True) for dy in (0, 3, 1, 2))[1:]


def latent_pieces(own):
    count = own.shape[0]
    up1 = send(own, "z", 8, 1)
    down1 = send(own, "z", 8, -1)
    up2 = send(own, "z", 8, 2)
    down2 = send(own, "z", 8, -2)
    up34 = send(join(up1, up2), "z", 8, 2)
    down3 = send(down1, "z", 8, -2)
    near = join(own, up1, down1, up2, down2)
    near_r = send(near, "x", 4, 1)
    near_l = send(near, "x", 4, -1)
    near_2 = send(near_r, "x", 4, 1)
    far = join(down3, up34)
    far_r = send(far, "x", 4, 1)
    far_l = send(far, "x", 4, -1)
    far_2 = send(far_l, "x", 4, -1)
    pieces = [near, near_r, near_l, near_2, far, far_r, far_l, far_2]
    table = []
    for offsets in ((0, 7, 1, 6, 2), (3, 5, 4)):
        for dx in (0, 3, 1, 2):
            table.append(tuple((i * count, count, dz, dx, 0) for i, dz in enumerate(offsets)))
    return pieces, tuple(table)


def per_device(query_latent, q_weight, key_absorb, value_up, branch_latent, lengths, row_depth):
    place = jnp.stack([lax.axis_index(a) for a in ("y", "core", "z", "x")]).astype(jnp.int32)
    pieces, table = latent_pieces(branch_latent[0])
    weights = weight_pieces(q_weight)
    query, seen, rank = project(lengths, place, row_depth[None], query_latent, weights, key_absorb)
    return attend(place, query, seen, rank, value_up, pieces, table)


def solution(mesh):
    torus = Mesh(mesh.devices.reshape(4, 2, 8, 4), ("y", "core", "z", "x"))
    group, head = ("y", "core"), ("z", "x")
    in_specs = (
        P(group, None),
        P(group, head),
        P(head, None, None),
        P(head, None, None),
        P(group, head, None),
        P(group),
        P(group),
    )
    return jax.shard_map(
        per_device, mesh=torus, in_specs=in_specs, out_specs=P(group, head), check_vma=False
    )
```

```python
import math

import jax
import jax.numpy as jnp
from jax import lax
from jax.experimental import pallas as pl
from jax.experimental.pallas import tpu as pltpu
from jax.sharding import Mesh
from jax.sharding import PartitionSpec as P


NOPE = 128
ROPE = 64
KVR = 512
VDIM = 128
WIDTH = KVR + ROPE
QDIM = NOPE + ROPE
LMAX = 1536
ROWS = 512
HEADS = 4
RB = 128
NRB = ROWS // RB
M = RB * HEADS
PB = 256
NPB = LMAX // PB
MASKED = -1e30
SCALE2 = (NOPE + ROPE) ** (-0.5) * math.log2(math.e)
F32 = jnp.float32
BF16 = jnp.bfloat16
NT = (((1,), (1,)), ((), ()))


def iota(shape, dim):
    return lax.broadcasted_iota(jnp.int32, shape, dim).astype(F32)


def weight_row(place_ref, dy, other):
    core = 1 - place_ref[1] if other else place_ref[1]
    return pl.multiple_of(lax.rem(place_ref[0] + dy, 4) * 384 + core * 192, 64)


def project_body(limit_ref, place_ref, ql_hbm, own_hbm, depth_hbm, *refs):
    pieces = refs[: len(WEIGHT_PIECES)]
    absorb_hbm, out_ref, seen_ref, rank_ref, weight, ql_ref, absorb_ref, depth_ref, arrived = refs[len(WEIGHT_PIECES) :]
    own_rows = weight.at[pl.ds(weight_row(place_ref, 0, False), 192), :]
    fetches = [
        pltpu.make_async_copy(depth_hbm, depth_ref, arrived.at[0]),
        pltpu.make_async_copy(own_hbm, own_rows, arrived.at[1]),
        pltpu.make_async_copy(ql_hbm, ql_ref, arrived.at[2]),
        pltpu.make_async_copy(absorb_hbm, absorb_ref, arrived.at[3]),
    ]
    for fetch in fetches:
        fetch.start()
    for ref, (dy, other) in zip(pieces, WEIGHT_PIECES, strict=True):
        weight[pl.ds(weight_row(place_ref, dy, other), 192), :] = ref[...]
    fetches[0].wait()
    seen = jnp.minimum(depth_ref[...], limit_ref[0]).astype(F32)
    rows = iota((ROWS, ROWS), 0)
    cols = iota((ROWS, ROWS), 1)
    key_row = jnp.broadcast_to(seen * ROWS, (ROWS, ROWS)) + cols
    diagonal = rows == cols
    key_col = jnp.sum(jnp.where(diagonal, key_row, 0.0), axis=1, keepdims=True)
    below = jnp.where(key_col < key_row, 1.0, 0.0)
    rank_row = jnp.sum(below, axis=0, keepdims=True)
    rank_ref[...] = jnp.sum(jnp.where(key_row < key_col, 1.0, 0.0), axis=1, keepdims=True)
    chosen = rows == rank_row
    seen_ref[...] = jnp.sum(jnp.where(chosen, seen, 0.0), axis=1, keepdims=True)
    order = jnp.where(chosen, 1.0, 0.0).astype(BF16)
    fetches[1].wait()
    fetches[2].wait()
    query = jnp.dot(ql_ref[...], weight[...], preferred_element_type=F32).astype(BF16)
    query = jnp.dot(order, query, preferred_element_type=F32).astype(BF16)
    fetches[3].wait()
    for h in range(HEADS):
        nope = query[:, h * QDIM : h * QDIM + NOPE]
        rope = query[:, h * QDIM + NOPE : (h + 1) * QDIM]
        lat = jnp.dot(nope, absorb_ref[h], preferred_element_type=F32).astype(BF16)
        for b in range(NRB):
            out_ref[b, h, :, :KVR] = lat[b * RB : (b + 1) * RB]
            out_ref[b, h, :, KVR:] = rope[b * RB : (b + 1) * RB]


def join_body(*refs):
    row = 0
    for ref in refs[:-1]:
        refs[-1][row : row + ref.shape[0], :] = ref[...]
        row += ref.shape[0]


def attend_body(n_pieces, table, place_ref, query_ref, seen_ref, rank_ref, value_ref, *refs):
    pieces = refs[:n_pieces]
    out_ref, latent, score, seen_wide, peak, total, acc, result = refs[n_pieces:]
    z, x = place_ref[2], place_ref[3]
    for ref, blocks in zip(pieces, table, strict=True):
        for row, size, dz, dx, skip in blocks:
            start = (lax.rem(z + dz, 8) * 4 + lax.rem(x + dx, 4)) * 48 + skip
            latent[pl.ds(pl.multiple_of(start, 8), size), :] = ref[row : row + size, :]
    lanes = iota((M, 128), 1)

    def block(b, carry):
        base = pl.multiple_of(b * RB, RB)
        seen = jnp.broadcast_to(seen_ref[pl.ds(base, RB), :], (RB, 128))
        most = jnp.max(seen)
        count = (most.astype(jnp.int32) + (PB - 1)) // PB
        seen_wide[...] = jnp.concatenate([seen] * HEADS, axis=0)

        def scores(i, first):
            start = i * PB
            s = lax.dot_general(
                query_ref[b].reshape(M, WIDTH), latent[pl.ds(start, PB), :], NT, preferred_element_type=F32
            )
            halves = []
            for j in range(PB // 128):
                at = lanes + float(start + 128 * j)
                half = jnp.where(at < seen_wide[...], s[:, 128 * j : 128 * (j + 1)], MASKED)
                score[i, :, 128 * j : 128 * (j + 1)] = half
                halves.append(half)
            best = halves[0]
            for half in halves[1:]:
                best = jnp.maximum(best, half)
            peak[...] = best if first else jnp.maximum(peak[...], best)

        def values(i, first):
            start = i * PB
            parts = [
                jnp.exp2((score[i, :, 128 * j : 128 * (j + 1)] - peak[...]) * SCALE2) for j in range(PB // 128)
            ]
            add = parts[0]
            for part in parts[1:]:
                add = add + part
            total[...] = add if first else total[...] + add
            weights = jnp.concatenate([part.astype(BF16) for part in parts], axis=1)
            more = jnp.dot(weights, latent[pl.ds(start, PB), :KVR], preferred_element_type=F32)
            acc[...] = more if first else acc[...] + more

        def widen():
            peak[...] = jnp.broadcast_to(jnp.max(peak[...], axis=1, keepdims=True), (M, 128))

        def finish():
            inverse = 1.0 / jnp.sum(total[...], axis=1, keepdims=True)
            context = (acc[...] * inverse).astype(BF16)
            for h in range(HEADS):
                result[pl.ds(base, RB), h * VDIM : (h + 1) * VDIM] = jnp.dot(
                    context[h * RB : (h + 1) * RB], value_ref[h], preferred_element_type=F32
                ).astype(BF16)

        for n in range(1, NPB + 1):
            @pl.when(count == n)
            def _():
                for i in range(n):
                    scores(i, i == 0)
                widen()
                for i in range(n):
                    values(i, i == 0)
                finish()
        return carry

    lax.fori_loop(0, NRB, block, 0)
    back = jnp.where(iota((ROWS, ROWS), 1) == rank_ref[...], 1.0, 0.0).astype(BF16)
    out_ref[...] = jnp.dot(back, result[...], preferred_element_type=F32).astype(BF16)


SMEM = pl.BlockSpec(memory_space=pltpu.SMEM)
VMEM = pl.BlockSpec(memory_space=pltpu.VMEM)
HBM = pl.BlockSpec(memory_space=pltpu.HBM)


def call(body, smem, vmem, outs, scratch, flops, limit, far=()):
    one = len(outs) == 1
    return pl.pallas_call(
        body,
        in_specs=[SMEM] * len(smem) + [HBM if i in far else VMEM for i in range(len(vmem))],
        out_specs=VMEM if one else [VMEM] * len(outs),
        out_shape=outs[0] if one else outs,
        scratch_shapes=scratch,
        compiler_params=pltpu.CompilerParams(vmem_limit_bytes=limit),
        cost_estimate=pl.CostEstimate(flops=flops, transcendentals=0, bytes_accessed=1 << 20),
    )(*smem, *vmem)


def in_hbm(value):
    return pltpu.with_memory_space_constraint(value, pltpu.HBM)


def project(limit, place, depth, ql, pieces, absorb):
    column = jax.ShapeDtypeStruct((ROWS, 1), F32)
    return call(
        project_body, [limit, place],
        [in_hbm(ql), in_hbm(pieces[0]), in_hbm(depth), *pieces[1:], in_hbm(absorb)],
        [jax.ShapeDtypeStruct((NRB, HEADS, RB, WIDTH), BF16), column, column],
        [
            pltpu.VMEM((1536, HEADS * QDIM), BF16),
            pltpu.VMEM((ROWS, 1536), BF16),
            pltpu.VMEM((HEADS, NOPE, KVR), BF16),
            pltpu.VMEM((1, ROWS), jnp.int32),
            pltpu.SemaphoreType.DMA((4,)),
        ],
        2 * ROWS * 768 * (1536 + ROWS) + 2 * ROWS * HEADS * NOPE * KVR, 24 << 20, (0, 1, 2, len(pieces) + 2),
    )


def join(*pieces):
    count = sum(piece.shape[0] for piece in pieces)
    return call(join_body, [], list(pieces), [jax.ShapeDtypeStruct((count, WIDTH), BF16)], [], 1 << 20, 4 << 20)


def attend(place, query, seen, rank, value_up, pieces, table):
    body = lambda *refs: attend_body(len(pieces), table, *refs)
    return call(
        body, [place], [query, seen, rank, value_up, *pieces],
        [jax.ShapeDtypeStruct((ROWS, HEADS * VDIM), BF16)],
        [
            pltpu.VMEM((LMAX, WIDTH), BF16),
            pltpu.VMEM((NPB, M, PB), F32),
            pltpu.VMEM((M, 128), F32),
            pltpu.VMEM((M, 128), F32),
            pltpu.VMEM((M, 128), F32),
            pltpu.VMEM((M, KVR), F32),
            pltpu.VMEM((ROWS, HEADS * VDIM), BF16),
        ],
        2 * ROWS * HEADS * LMAX * (WIDTH + KVR), 30 << 20,
    )


def send(value, axis, size, step):
    return lax.ppermute(value, axis, [(i, (i + step) % size) for i in range(size)])


def weight_pieces(w):
    up = send(w, "y", 4, 1)
    down = send(w, "y", 4, -1)
    own2 = send(w, "core", 2, 1)
    far = send(up, "y", 4, 1)
    up2 = send(up, "core", 2, 1)
    down2 = send(down, "core", 2, 1)
    far2 = send(far, "core", 2, 1)
    return (w, up, down, far, own2, up2, down2, far2)


WEIGHT_PIECES = tuple((dy, other) for other in (False, True) for dy in (0, 3, 1, 2))[1:]


def latent_pieces(own):
    count = own.shape[0]
    up1 = send(own, "z", 8, 1)
    down1 = send(own, "z", 8, -1)
    up2 = send(own, "z", 8, 2)
    down2 = send(own, "z", 8, -2)
    up34 = send(join(up1, up2), "z", 8, 2)
    down3 = send(down1, "z", 8, -2)
    near = join(own, up1, down1, up2, down2)
    near_r = send(near, "x", 4, 1)
    near_l = send(near, "x", 4, -1)
    near_2 = send(near_r, "x", 4, 1)
    far = join(down3, up34)
    far_r = send(far, "x", 4, 1)
    far_l = send(far, "x", 4, -1)
    far_2 = send(far_l, "x", 4, -1)
    pieces = [near, near_r, near_l, near_2, far, far_r, far_l, far_2]
    table = []
    for offsets in ((0, 7, 1, 6, 2), (3, 5, 4)):
        for dx in (0, 3, 1, 2):
            table.append(tuple((i * count, count, dz, dx, 0) for i, dz in enumerate(offsets)))
    return pieces, tuple(table)


def per_device(query_latent, q_weight, key_absorb, value_up, branch_latent, lengths, row_depth):
    place = jnp.stack([lax.axis_index(a) for a in ("y", "core", "z", "x")]).astype(jnp.int32)
    pieces, table = latent_pieces(branch_latent[0])
    weights = weight_pieces(q_weight)
    query, seen, rank = project(lengths, place, row_depth[None], query_latent, weights, key_absorb)
    return attend(place, query, seen, rank, value_up, pieces, table)


def solution(mesh):
    torus = Mesh(mesh.devices.reshape(4, 2, 8, 4), ("y", "core", "z", "x"))
    group, head = ("y", "core"), ("z", "x")
    in_specs = (
        P(group, None),
        P(group, head),
        P(head, None, None),
        P(head, None, None),
        P(group, head, None),
        P(group),
        P(group),
    )
    return jax.shard_map(
        per_device, mesh=torus, in_specs=in_specs, out_specs=P(group, head), check_vma=False
    )
```
